32 devices in a mesh: spin: 1 (over z), depth: 4 (over y), row: 4 (over x), col: 2 (over core).
Axes of the slice: x: 4, y: 4, z: 1, core: 2. Of those that a mesh axis runs over, the one named last changes fastest.
The devices are a block of a 4x4x8 slice.
Arguments:
- hamiltonian: float32 [2, 3584, 3584], P('spin', 'row', 'col')
- spec_bounds: float32 [2, 2], P('spin')
- occ_count: int32 [2], P('spin')
Outputs:
- output 1: float32 [2, 3584, 3584], P('spin', 'row', 'col')
- output 2: float32 [2], P('spin')
All inputs are finite; a program needn't handle non-finite values.
Results may differ from the reference program's by a relative error of at most 0.001.
Values sent between devices are 32-bit elements.
A program may use at most 768 MiB of HBM per device.

```python
import jax
import jax.numpy as jnp
from jax import lax

ORDER = 3584
KPTS = 2
STEPS = 3


def setup_inputs(seed: int = 0, part: int = 0) -> dict:
    key_base = jax.random.fold_in(jax.random.key(seed), part)
    key_off, key_site, key_shift, key_margin, key_occ = jax.random.split(key_base, 5)
    raw_off = jax.random.normal(key_off, (KPTS, ORDER, ORDER), jnp.float32)
    coup_scale = (0.5 / ORDER) ** 0.5
    coupling = (raw_off + jnp.swapaxes(raw_off, 1, 2)) * coup_scale
    site_draw = jax.random.uniform(key_site, (KPTS, ORDER), jnp.float32)
    site_shift = jax.random.uniform(key_shift, (KPTS, 1), jnp.float32, -1.5, -0.5)
    onsite = site_shift + 0.8 * site_draw * site_draw
    identity = jnp.eye(ORDER, dtype=jnp.float32)
    hamiltonian = coupling + onsite[:, :, None] * identity
    margin = jax.random.uniform(key_margin, (KPTS, 2), jnp.float32, 0.1, 1.5)
    lower_bd = jnp.min(onsite, axis=1) - 2.0 - margin[:, 0]
    upper_bd = jnp.max(onsite, axis=1) + 2.0 + margin[:, 1]
    spec_bounds = jnp.stack([lower_bd, upper_bd], axis=1)
    occ_count = jax.random.randint(key_occ, (KPTS,), ORDER * 3 // 20, ORDER * 3 // 8 + 1, dtype=jnp.int32)
    return {'hamiltonian': hamiltonian, 'spec_bounds': spec_bounds, 'occ_count': occ_count}


def purify_one(operands):
    hamilton, bounds_one, occ_one = operands
    highest = lax.Precision.HIGHEST
    occupied = occ_one.astype(jnp.float32)
    chem_pot = jnp.trace(hamilton) / ORDER
    scale_fac = jnp.minimum(occupied / (bounds_one[1] - chem_pot), (ORDER - occupied) / (chem_pot - bounds_one[0]))
    identity = jnp.eye(ORDER, dtype=jnp.float32)
    start_dens = (scale_fac / ORDER) * (chem_pot * identity - hamilton) + (occupied / ORDER) * identity

    def purify_step(density, unused):
        dens_sq = jnp.dot(density, density, precision=highest, preferred_element_type=jnp.float32)
        dens_cube = jnp.dot(dens_sq, density, precision=highest, preferred_element_type=jnp.float32)
        tr_one = jnp.trace(density)
        tr_two = jnp.sum(density * density)
        tr_three = jnp.sum(dens_sq * density)
        purify_coef = (tr_two - tr_three) / (tr_one - tr_two)
        new_dens = ((1.0 - 2.0 * purify_coef) * density + (1.0 + purify_coef) * dens_sq - dens_cube) / (1.0 - purify_coef)
        return new_dens, None

    final_dens, unused_out = lax.scan(purify_step, start_dens, None, length=STEPS)
    energy = 2.0 * jnp.sum(final_dens * hamilton)
    return final_dens, energy


def reference(hamiltonian, spec_bounds, occ_count):
    density, energy = lax.map(purify_one, (hamiltonian, spec_bounds, occ_count))
    return density, energy
```

```python
import functools

import jax
import jax.numpy as jnp
from jax import lax
from jax.experimental import pallas as pl
from jax.experimental.pallas import tpu as pltpu
from jax.sharding import PartitionSpec as P

STEPS = 3
MESH = pl.DeviceIdType.MESH
LANE = 128
HIGHEST = lax.Precision.HIGHEST


class Geometry:
    def __init__(self, mesh, ham_shape):
        kpoints, self.blk, self.half = ham_shape
        self.depth = mesh.shape["depth"]
        self.rows = mesh.shape["row"]
        self.cols = mesh.shape["col"]
        self.kpoints = kpoints
        self.layers = self.depth // kpoints
        self.order = self.half * self.cols
        self.strip = self.blk // (self.layers * self.cols)
        self.lo = self.blk // 2 // LANE * LANE
        self.wide = self.blk - self.lo
        assert self.rows == 4 and self.cols == 2 and self.layers == 2 and self.depth == 4


def rem(a, b):
    return lax.rem(a, b)


def gather_kernel(geo, strip_ref, full_ref, send_sem, recv_sem, sib_send, sib_recv, local_sem):
    d = lax.axis_index("depth")
    r = lax.axis_index("row")
    c = lax.axis_index("col")
    e = rem(d, geo.layers)
    mate = d + 1 - 2 * e
    up, down = rem(r + 1, 4), rem(r + 3, 4)
    to_up, to_down, to_mate = {"row": up}, {"row": down}, {"depth": mate}
    to_sib = {"col": 1 - c}

    barrier = pltpu.get_barrier_semaphore()
    for dev in (to_up, to_down, to_mate, to_sib):
        pl.semaphore_signal(barrier, inc=1, device_id=dev, device_id_type=MESH)
    pl.semaphore_wait(barrier, 4)

    hh = geo.strip // 2

    def place(lam, delta, h, part, core):
        rr = rem(r + delta, 4)
        ee = e if lam == 0 else 1 - e
        row0 = rr * geo.blk + (ee * 2 + core) * geo.strip
        size = geo.strip
        if h is not None:
            row0, size = row0 + h * hh, hh
        if part < 2:
            col0, width = rem(rr + part, 4) * geo.blk, geo.blk
        else:
            col0 = rem(rr + 2, 4) * geo.blk + geo.lo * rem(rr // 2 + ee, 2)
            width = geo.wide
        return (pl.ds(pl.multiple_of(row0, 8), size), pl.ds(pl.multiple_of(col0, LANE), width))

    slots = {(lam, delta, h): i for i, (lam, delta, h) in enumerate(
        [(lam, delta, h) for lam in (0, 1) for delta, h in ((0, None), (1, None), (3, None), (2, 0), (2, 1))])}

    def branch(core):
        started = []

        def send(src, there, dev, part, n):
            here = place(*src, part, core)
            if src == (0, 0, None):
                rows, cols = here
                ref = strip_ref.at[:, cols]
            else:
                ref = full_ref.at[here]
            cp = pltpu.make_async_remote_copy(
                src_ref=ref, dst_ref=full_ref.at[here],
                send_sem=send_sem.at[n, part], recv_sem=recv_sem.at[slots[there], part],
                device_id=dev, device_id_type=MESH)
            cp.start()
            started.append(cp)

        def sib(slot, part):
            here = place(*slot, part, core)
            ref = strip_ref.at[:, here[1]] if slot == (0, 0, None) else full_ref.at[here]
            cp = pltpu.make_async_remote_copy(
                src_ref=ref, dst_ref=full_ref.at[here],
                send_sem=sib_send.at[slots[slot], part], recv_sem=sib_recv.at[slots[slot], part],
                device_id=to_sib, device_id_type=MESH)
            cp.start()
            started.append(cp)

        def half(slot, h):
            return (slot[0], slot[1], h)

        def arrive(slot, part):
            here = place(*slot, part, core)
            pltpu.make_async_copy(full_ref.at[here], full_ref.at[here], recv_sem.at[slots[slot], part]).wait()

        def send_half(src, h, there, dev, part, n):
            rr_src = (src[0], src[1], h)
            here = place(*rr_src, part, core)
            cp = pltpu.make_async_remote_copy(
                src_ref=full_ref.at[here], dst_ref=full_ref.at[here],
                send_sem=send_sem.at[n, part], recv_sem=recv_sem.at[slots[there], part],
                device_id=dev, device_id_type=MESH)
            cp.start()
            started.append(cp)

        own, mate_own = (0, 0, None), (1, 0, None)
        below = lambda lam: (lam, 3, None)
        above = lambda lam: (lam, 1, None)
        far = lambda lam, h: (lam, 2, h)
        for p in range(3):
            send(own, mate_own, to_mate, p, 0)
            send(own, below(0), to_up, p, 1)
            send(own, above(0), to_down, p, 2)
        for p in range(3):
            sib(own, p)
        if core == 0:
            for p in range(3):
                arrive(mate_own, p)
                send(mate_own, below(1), to_up, p, 3)
                send(mate_own, above(1), to_down, p, 4)
                sib(mate_own, p)
            for lam in (0, 1):
                for p in range(3):
                    arrive(below(lam), p)
                    send_half(below(lam), 0, far(lam, 0), to_up, p, 5 + 2 * lam)
                    sib(below(lam), p)
                    arrive(above(lam), p)
                    send_half(above(lam), 1, far(lam, 1), to_down, p, 6 + 2 * lam)
                    sib(above(lam), p)
            for lam in (0, 1):
                for p in range(3):
                    for h in (0, 1):
                        arrive(far(lam, h), p)
                        sib(far(lam, h), p)
        else:
            for p in range(3):
                arrive(below(0), p)
                send_half(below(0), 0, far(0, 0), to_up, p, 3)
                send(below(0), below(1), to_mate, p, 4)
                sib(below(0), p)
                arrive(above(0), p)
                send_half(above(0), 1, far(0, 1), to_down, p, 5)
                send(above(0), above(1), to_mate, p, 6)
                sib(above(0), p)
            for p in range(3):
                arrive(mate_own, p)
                sib(mate_own, p)
            for p in range(3):
                for h in (0, 1):
                    arrive(far(0, h), p)
                    send(far(0, h), far(1, h), to_mate, p, 7 + h)
                    sib(far(0, h), p)
            for p in range(3):
                for slot in (below(1), above(1)):
                    arrive(slot, p)
                    sib(slot, p)
            for p in range(3):
                for h in (0, 1):
                    arrive(far(1, h), p)
                    sib(far(1, h), p)
        for slot in slots:
            for p in range(3):
                here = place(*slot, p, 1 - core)
                pltpu.make_async_copy(full_ref.at[here], full_ref.at[here], sib_recv.at[slots[slot], p]).wait()
        for cp in started:
            cp.wait_send()

    row0 = r * geo.blk + (e * 2 + c) * geo.strip
    keep = pltpu.make_async_copy(strip_ref, full_ref.at[pl.ds(pl.multiple_of(row0, 8), geo.strip)], local_sem)
    keep.start()
    pl.when(c == 0)(lambda: branch(0))
    pl.when(c == 1)(lambda: branch(1))
    keep.wait()


def gather(geo, strip, call):
    return pl.pallas_call(
        functools.partial(gather_kernel, geo),
        out_shape=jax.ShapeDtypeStruct((geo.order, geo.order), jnp.float32),
        in_specs=[pl.BlockSpec(memory_space=pltpu.VMEM)],
        out_specs=pl.BlockSpec(memory_space=pl.ANY),
        scratch_shapes=[
            pltpu.SemaphoreType.DMA((9, 3)),
            pltpu.SemaphoreType.DMA((10, 3)),
            pltpu.SemaphoreType.DMA((10, 3)),
            pltpu.SemaphoreType.DMA((10, 3)),
            pltpu.SemaphoreType.DMA,
        ],
        compiler_params=pltpu.CompilerParams(collective_id=call, has_side_effects=True),
        name="gather",
    )(strip)


def mirror(geo, full):
    blk, lo, wide = geo.blk, geo.lo, geo.wide
    per = blk // LANE
    shape = jax.ShapeDtypeStruct(full.shape, full.dtype)

    def body(src_ref, dst_ref):
        dst_ref[...] = src_ref[...].T

    full = pl.pallas_call(
        body, grid=(4, per), out_shape=shape,
        in_specs=[pl.BlockSpec((LANE, blk), lambda i, t: (i * per + t, (i + 1) % 4))],
        out_specs=pl.BlockSpec((blk, LANE), lambda i, t: ((i + 1) % 4, i * per + t)),
        input_output_aliases={0: 0}, name="mirror_next",
    )(full)

    def rows_of(i, t):
        return pl.multiple_of(i * blk + t * wide, LANE)

    def cols_of(i, t):
        return pl.multiple_of((i + 2) % 4 * blk + lo * ((i // 2 + t) % 2), LANE)

    return pl.pallas_call(
        body, grid=(4, 2), out_shape=shape,
        in_specs=[pl.BlockSpec((pl.Element(lo), pl.Element(wide)), lambda i, t: (rows_of(i, t), cols_of(i, t)))],
        out_specs=pl.BlockSpec((pl.Element(wide), pl.Element(lo)), lambda i, t: (cols_of(i, t), rows_of(i, t))),
        input_output_aliases={0: 0}, name="mirror_far",
    )(full)


def spread_kernel(geo, strip_ref, out_ref, send_sem, recv_sem, sib_send, sib_recv, local_sem):
    d = lax.axis_index("depth")
    c = lax.axis_index("col")
    up, down = {"depth": rem(d + 1, 4)}, {"depth": rem(d + 3, 4)}
    to_sib = {"col": 1 - c}
    barrier = pltpu.get_barrier_semaphore()
    for dev in (up, down, to_sib):
        pl.semaphore_signal(barrier, inc=1, device_id=dev, device_id_type=MESH)
    pl.semaphore_wait(barrier, 3)

    hh = geo.strip // 2

    def place(delta, core, h):
        dd = rem(d + delta, 4)
        row0 = (rem(dd, geo.layers) * 2 + core) * geo.strip
        size = geo.strip
        if h is not None:
            row0, size = row0 + h * hh, hh
        return (dd // geo.layers, pl.ds(pl.multiple_of(row0, 8), size))

    slots = {(0, None): 0, (1, None): 1, (3, None): 2, (2, 0): 3, (2, 1): 4}
    mine = pl.ds(pl.multiple_of(c * geo.half, LANE), geo.half)
    other = pl.ds(pl.multiple_of((1 - c) * geo.half, LANE), geo.half)
    started = []

    def send(src, dst, there, who, dev, n):
        cp = pltpu.make_async_remote_copy(
            src_ref=src, dst_ref=dst, send_sem=send_sem.at[n, who], recv_sem=recv_sem.at[slots[there], who],
            device_id=dev, device_id_type=MESH)
        cp.start()
        started.append(cp)

    cp = pltpu.make_async_remote_copy(
        src_ref=strip_ref.at[:, other], dst_ref=out_ref.at[place(0, c, None)], send_sem=sib_send, recv_sem=sib_recv,
        device_id=to_sib, device_id_type=MESH)
    cp.start()
    started.append(cp)
    keep = pltpu.make_async_copy(strip_ref.at[:, mine], out_ref.at[place(0, c, None)], local_sem)
    keep.start()
    own = out_ref.at[place(0, c, None)]
    send(strip_ref.at[:, mine], own, (3, None), 0, up, 0)
    send(strip_ref.at[:, mine], own, (1, None), 0, down, 1)
    sibs = out_ref.at[place(0, 1 - c, None)]
    pltpu.make_async_copy(sibs, sibs, sib_recv).wait()
    send(sibs, sibs, (3, None), 1, up, 0)
    send(sibs, sibs, (1, None), 1, down, 1)

    def arrive(delta, h, who):
        ref = out_ref.at[place(delta, c if who == 0 else 1 - c, h)]
        pltpu.make_async_copy(ref, ref, recv_sem.at[slots[(delta, h)], who]).wait()

    for who in (0, 1):
        core = c if who == 0 else 1 - c
        arrive(3, None, who)
        ref = out_ref.at[place(3, core, 0)]
        send(ref, ref, (2, 0), who, up, 2)
        arrive(1, None, who)
        ref = out_ref.at[place(1, core, 1)]
        send(ref, ref, (2, 1), who, down, 3)
    for who in (0, 1):
        arrive(2, 0, who)
        arrive(2, 1, who)
    keep.wait()
    for cp in started:
        cp.wait_send()


def spread(geo, strip, call):
    return pl.pallas_call(
        functools.partial(spread_kernel, geo),
        out_shape=jax.ShapeDtypeStruct((geo.kpoints, geo.blk, geo.half), jnp.float32),
        in_specs=[pl.BlockSpec(memory_space=pltpu.VMEM)],
        out_specs=pl.BlockSpec(memory_space=pl.ANY),
        scratch_shapes=[
            pltpu.SemaphoreType.DMA((4, 2)),
            pltpu.SemaphoreType.DMA((5, 2)),
            pltpu.SemaphoreType.DMA,
            pltpu.SemaphoreType.DMA,
            pltpu.SemaphoreType.DMA,
        ],
        compiler_params=pltpu.CompilerParams(collective_id=call, has_side_effects=True),
        name="spread",
    )(strip)


def solution(mesh):
    def local_purify(ham, spec_bounds, occ_count):
        geo = Geometry(mesh, ham.shape)
        n = geo.order
        d = lax.axis_index("depth")
        r = lax.axis_index("row")
        c = lax.axis_index("col")
        m, e = d // geo.layers, d % geo.layers
        per_col = geo.rows // geo.cols
        on_diag = (r // per_col) == c
        diag_start = (r % per_col) * geo.blk
        square = lax.dynamic_slice_in_dim(ham, diag_start, geo.blk, axis=2)
        tr = jnp.where(on_diag, jnp.trace(square, axis1=1, axis2=2), 0.0)
        mu = lax.psum(tr, ("row", "col")) / n
        occ = occ_count.astype(jnp.float32)
        lam = jnp.minimum(occ / (spec_bounds[:, 1] - mu), (n - occ) / (mu - spec_bounds[:, 0]))
        add = (lam * mu + occ) / n
        scale = lam / n

        row0 = r * geo.blk + (e * 2 + c) * geo.strip
        rows = lax.broadcasted_iota(jnp.int32, (geo.strip, n), 0) + row0
        cols = lax.broadcasted_iota(jnp.int32, (geo.strip, n), 1)
        diag = rows == cols

        ham_m = lax.dynamic_index_in_dim(ham, m, axis=0, keepdims=False)
        layer_rows = lax.dynamic_slice_in_dim(ham_m, e * 2 * geo.strip, 2 * geo.strip, axis=0)
        layer_all = lax.all_gather(layer_rows, "col", axis=1, tiled=True)
        ham_strip = lax.dynamic_slice_in_dim(layer_all, c * geo.strip, geo.strip, axis=0)
        strip = jnp.where(diag, add[m], 0.0) - scale[m] * ham_strip

        for step in range(STEPS):
            full = mirror(geo, gather(geo, strip, step))
            sq = jnp.dot(strip, full, precision=HIGHEST, preferred_element_type=jnp.float32)
            sums = jnp.stack([jnp.sum(jnp.where(diag, strip, 0.0)), jnp.sum(strip * strip), jnp.sum(sq * strip)])
            slot = (jnp.arange(geo.kpoints) == m).astype(jnp.float32)
            traces = lax.psum(slot[:, None] * sums[None, :], ("depth", "row", "col"))
            t = lax.dynamic_index_in_dim(traces, m, axis=0, keepdims=False)
            coef = (t[1] - t[2]) / (t[0] - t[1])
            cube = jnp.dot(sq, full, precision=HIGHEST, preferred_element_type=jnp.float32)
            strip = ((1.0 - 2.0 * coef) * strip + (1.0 + coef) * sq - cube) / (1.0 - coef)
        density = spread(geo, strip, STEPS)
        energy = 2.0 * lax.psum(jnp.sum(density * ham, axis=(1, 2)), ("row", "col"))
        return density, energy

    mat = P("spin", "row", "col")
    return jax.shard_map(
        local_purify, mesh=mesh, in_specs=(mat, P("spin", None), P("spin")), out_specs=(mat, P("spin")), check_vma=False)
```

```python
import functools

import jax
import jax.numpy as jnp
from jax import lax
from jax.experimental import pallas as pl
from jax.experimental.pallas import tpu as pltpu
from jax.sharding import PartitionSpec as P

STEPS = 3
MESH = pl.DeviceIdType.MESH
LANE = 128
HIGHEST = lax.Precision.HIGHEST


class Geometry:
    def __init__(self, mesh, ham_shape):
        kpoints, self.blk, self.half = ham_shape
        self.depth = mesh.shape["depth"]
        self.rows = mesh.shape["row"]
        self.cols = mesh.shape["col"]
        self.kpoints = kpoints
        self.layers = self.depth // kpoints
        self.order = self.half * self.cols
        self.strip = self.blk // (self.layers * self.cols)
        self.lo = self.blk // 2 // LANE * LANE
        self.wide = self.blk - self.lo
        self.chunk = 4 * LANE
        self.chunks = self.order // self.chunk
        assert self.rows == 4 and self.cols == 2 and self.layers == 2 and self.depth == 4


def rem(a, b):
    return lax.rem(a, b)


class Links:
    def __init__(self, geo, own_ref, full_ref, send_sem, recv_sem, sib_send, sib_recv):
        self.geo, self.own, self.full = geo, own_ref, full_ref
        self.send_sem, self.recv_sem, self.sib_send, self.sib_recv = send_sem, recv_sem, sib_send, sib_recv
        d = lax.axis_index("depth")
        self.r = lax.axis_index("row")
        self.c = lax.axis_index("col")
        self.e = rem(d, geo.layers)
        self.up, self.down = {"row": rem(self.r + 1, 4)}, {"row": rem(self.r + 3, 4)}
        self.mate = {"depth": d + 1 - 2 * self.e}
        self.sibling = {"col": 1 - self.c}
        self.drained = set()
        self.slots = {slot: i for i, slot in enumerate(
            [(lam, delta, h) for lam in (0, 1) for delta, h in ((0, None), (1, None), (3, None), (2, 0), (2, 1))])}

    def place(self, slot, part, core):
        geo = self.geo
        lam, delta, h = slot
        rr = rem(self.r + delta, 4)
        ee = self.e if lam == 0 else 1 - self.e
        row0 = rr * geo.blk + (ee * 2 + core) * geo.strip
        size = geo.strip
        if h is not None:
            row0, size = row0 + h * (geo.strip // 2), geo.strip // 2
        if part < 2:
            col0, width = rem(rr + part, 4) * geo.blk, geo.blk
        else:
            col0 = rem(rr + 2, 4) * geo.blk + geo.lo * rem(rr // 2 + ee, 2)
            width = geo.wide
        return pl.ds(pl.multiple_of(row0, 8), size), pl.ds(pl.multiple_of(col0, LANE), width)

    def copy(self, src, there, dev, part, core, n):
        here = self.place(src, part, core)
        ref = self.own.at[:, here[1]] if src == OWN else self.full.at[here]
        return pltpu.make_async_remote_copy(
            src_ref=ref, dst_ref=self.full.at[here], send_sem=self.send_sem.at[n, part],
            recv_sem=self.recv_sem.at[self.slots[there], part], device_id=dev, device_id_type=MESH)

    def sib_copy(self, slot, part, core):
        here = self.place(slot, part, core)
        ref = self.own.at[:, here[1]] if slot == OWN else self.full.at[here]
        i = self.slots[slot]
        return pltpu.make_async_remote_copy(
            src_ref=ref, dst_ref=self.full.at[here], send_sem=self.sib_send.at[i, part],
            recv_sem=self.sib_recv.at[i, part], device_id=self.sibling, device_id_type=MESH)

    def arrive(self, slot, part, core):
        here = self.full.at[self.place(slot, part, core)]
        pltpu.make_async_copy(here, here, self.recv_sem.at[self.slots[slot], part]).wait()

    def sib_arrive(self, slot, part, core):
        here = self.full.at[self.place(slot, part, 1 - core)]
        pltpu.make_async_copy(here, here, self.sib_recv.at[self.slots[slot], part]).wait()

    def sends(self, core):
        table = [(OWN, MATE, self.mate), (OWN, below(0), self.up), (OWN, above(0), self.down)]
        lams = (0, 1) if core == 0 else (0,)
        if core == 0:
            table += [(MATE, below(1), self.up), (MATE, above(1), self.down)]
        for lam in lams:
            table += [((lam, 3, 0), far(lam, 0), self.up), ((lam, 1, 1), far(lam, 1), self.down)]
        if core == 1:
            table += [(below(0), below(1), self.mate), (above(0), above(1), self.mate)]
            table += [(far(0, h), far(1, h), self.mate) for h in (0, 1)]
        return table

    def forward(self, slot, part, core):
        for n, (src, there, dev) in enumerate(self.sends(core)):
            if src == slot or (slot[2] is None and slot[1] in (1, 3) and src[:2] == slot[:2] and src[2] is not None):
                self.copy(src, there, dev, part, core, n).start()
        self.sib_copy(slot, part, core).start()

    def relay(self, slot, part, core):
        self.arrive(slot, part, core)
        self.forward(slot, part, core)

    def drain(self, slots, parts, core):
        for part in parts:
            for n, (src, there, dev) in enumerate(self.sends(core)):
                whole = src[:2] + ((None,) if src[1] != 2 else (src[2],))
                if whole in slots and (core, n, part) not in self.drained:
                    self.drained.add((core, n, part))
                    self.copy(src, there, dev, part, core, n).wait_send()
            for slot in slots:
                if (core, slot, part) not in self.drained:
                    self.drained.add((core, slot, part))
                    self.sib_copy(slot, part, core).wait_send()


OWN, MATE = (0, 0, None), (1, 0, None)


def below(lam):
    return (lam, 3, None)


def above(lam):
    return (lam, 1, None)


def far(lam, h):
    return (lam, 2, h)


def per_core(c, fn):
    pl.when(c == 0)(lambda: fn(0))
    pl.when(c == 1)(lambda: fn(1))


class Reduce:
    def __init__(self, geo, src, mid, box, send, recv):
        self.src, self.mid, self.box, self.send, self.recv = src, mid, box, send, recv
        d, r, c = (lax.axis_index(a) for a in ("depth", "row", "col"))
        mate = d + 1 - 2 * rem(d, geo.layers)
        self.round1 = [{"row": rem(r + k, 4)} for k in (1, 2, 3)]
        self.round2 = [{"depth": mate}, {"col": 1 - c}, {"depth": mate, "col": 1 - c}]

    def copies(self, first):
        devs, src, base = (self.round1, self.src, 0) if first else (self.round2, self.mid, 3)
        return [pltpu.make_async_remote_copy(
            src_ref=src, dst_ref=self.box.at[base + i], send_sem=self.send.at[base + i], recv_sem=self.recv.at[base + i],
            device_id=dev, device_id_type=MESH) for i, dev in enumerate(devs)]

    def start(self, first):
        for cp in self.copies(first):
            cp.start()

    def total(self, first):
        for cp in self.copies(first):
            cp.wait()
        base = 0 if first else 3
        src = self.src if first else self.mid
        return (src[...] + self.box[base]) + (self.box[base + 1] + self.box[base + 2])


def enter(devs):
    barrier = pltpu.get_barrier_semaphore()
    for dev in devs:
        pl.semaphore_signal(barrier, inc=1, device_id=dev, device_id_type=MESH)
    pl.semaphore_wait(barrier, len(devs))


def transpose_region(full, row0, col0, h, w, tin, tout, sem):
    rows, cols = pl.ds(pl.multiple_of(row0, LANE), h), pl.ds(pl.multiple_of(col0, LANE), w)
    cp = pltpu.make_async_copy(full.at[rows, cols], tin.at[pl.ds(0, h), pl.ds(0, w)], sem)
    cp.start()
    cp.wait()

    def body(t, carry):
        at = pl.ds(pl.multiple_of(t * LANE, LANE), LANE)
        tout[pl.ds(0, w), at] = tin[at, pl.ds(0, w)].T
        return carry

    lax.fori_loop(0, h // LANE, body, 0)
    out = full.at[pl.ds(pl.multiple_of(col0, LANE), w), pl.ds(pl.multiple_of(row0, LANE), h)]
    cp = pltpu.make_async_copy(tout.at[pl.ds(0, w), pl.ds(0, h)], out, sem)
    cp.start()
    cp.wait()


def mirror_next(geo, full, k, tin, tout, sem):
    k = rem(k, 4)
    transpose_region(full, k * geo.blk, rem(k + 1, 4) * geo.blk, geo.blk, geo.blk, tin, tout, sem)


def mirror_far(geo, full, k, tin, tout, sem):
    def body(j, carry):
        i, t = rem(k + 2 * (j // 2), 4), rem(j, 2)
        row0 = i * geo.blk + t * geo.wide
        col0 = rem(i + 2, 4) * geo.blk + geo.lo * rem(i // 2 + t, 2)
        transpose_region(full, row0, col0, geo.lo, geo.wide, tin, tout, sem)
        return carry

    lax.fori_loop(0, 4, body, 0)


def complete(geo, links, core, keeps, tin, tout, sem, done):
    full, r = links.full, links.r
    near = (MATE,) if core == 0 else (below(0), above(0))
    for part in range(done, 3):
        for slot in near:
            links.relay(slot, part, core)
    if core == 0:
        for lam in (0, 1):
            for part in range(3):
                links.relay(below(lam), part, core)
                links.relay(above(lam), part, core)
    else:
        for part in range(3):
            links.relay(MATE, part, core)
        for part in range(3):
            for h in (0, 1):
                links.relay(far(0, h), part, core)
    for cp in keeps:
        cp.wait()

    def sibs(slots):
        for slot in slots:
            for part in range(3):
                links.sib_arrive(slot, part, core)

    sibs((OWN, MATE))
    mirror_next(geo, full, r, tin, tout, sem)
    if core == 1:
        for part in range(3):
            links.relay(below(1), part, core)
            links.relay(above(1), part, core)
    sibs((below(0), below(1), above(0), above(1)))
    mirror_next(geo, full, r + 3, tin, tout, sem)
    mirror_next(geo, full, r + 1, tin, tout, sem)
    links.drain((below(0), below(1), above(0), above(1)), (2,), core)
    mirror_far(geo, full, r + 1, tin, tout, sem)
    for part in range(3):
        for lam in (0, 1) if core == 0 else (1,):
            for h in (0, 1):
                links.relay(far(lam, h), part, core)
    sibs([far(lam, h) for lam in (0, 1) for h in (0, 1)])
    mirror_next(geo, full, r + 2, tin, tout, sem)
    links.drain([slot for slot in links.slots if slot[1] in (0, 2)], (2,), core)
    mirror_far(geo, full, r, tin, tout, sem)
    links.drain(list(links.slots), range(3), core)


def keep_copy(links, own, part, sem):
    geo = links.geo
    row0 = links.r * geo.blk + (links.e * 2 + links.c) * geo.strip
    cols = pl.ds(pl.multiple_of(rem(links.r + part, 4) * geo.blk, LANE), geo.blk)
    return pltpu.make_async_copy(own.at[:, cols], links.full.at[pl.ds(pl.multiple_of(row0, 8), geo.strip), cols], sem.at[part])


def first_kernel(geo, strip, full, send_sem, recv_sem, sib_send, sib_recv, keep_sem, tin, tout, tsem):
    links = Links(geo, strip, full, send_sem, recv_sem, sib_send, sib_recv)
    enter([links.up, links.down, links.mate, links.sibling])
    keeps = [keep_copy(links, strip, part, keep_sem) for part in range(4)]

    def run(core):
        for part in range(3):
            links.forward(OWN, part, core)
        for cp in keeps:
            cp.start()
        complete(geo, links, core, keeps, tin, tout, tsem, 0)

    per_core(links.c, run)


def cube_loop(geo, red, first_block, full_in, sq, strip, new, buf, acc, buf_sem, hook):
    per, size, blk = geo.chunks, geo.chunk, geo.blk

    def cols_of(part):
        return pl.ds(pl.multiple_of(rem(first_block + part, 4) * blk, LANE), blk)

    def load(i):
        rows = pl.ds(pl.multiple_of(rem(i, per) * size, LANE), size)
        slot = rem(i, 2)
        return pltpu.make_async_copy(full_in.at[rows, cols_of(i // per)], buf.at[slot], buf_sem.at[slot])

    load(0).start()

    def body(i, carry):
        k = rem(i, per)

        @pl.when(i + 1 < 4 * per)
        def _():
            load(i + 1).start()

        load(i).wait()

        @pl.when(k == 0)
        def _():
            acc[...] = jnp.zeros_like(acc)

        acc[...] += jnp.dot(sq[:, pl.ds(pl.multiple_of(k * size, LANE), size)], buf[rem(i, 2)],
                            precision=HIGHEST, preferred_element_type=jnp.float32)

        @pl.when(i == 1)
        def _():
            red.mid[...] = red.total(True)

        @pl.when(i == 3)
        def _():
            red.start(False)

        @pl.when(i == per - 1)
        def _():
            red.src_total[...] = red.total(False)

        @pl.when(k == per - 1)
        def _():
            cols = cols_of(i // per)
            t1, t2, t3 = (red.src_total[j:j + 1, 0:1] for j in range(3))
            coef = (t2 - t3) / (t1 - t2)
            new[:, cols] = ((1.0 - 2.0 * coef) * strip[:, cols] + (1.0 + coef) * sq[:, cols] - acc[...]) / (1.0 - coef)

        hook(i)
        return carry

    lax.fori_loop(0, 4 * per, body, 0)


def mid_kernel(geo, full_in, sq, strip, sums, full, new, send_sem, recv_sem, sib_send, sib_recv, keep_sem, tin, tout, tsem,
               buf, acc, buf_sem, mid, tot, box, red_send, red_recv):
    links = Links(geo, new, full, send_sem, recv_sem, sib_send, sib_recv)
    red = Reduce(geo, sums, mid, box, red_send, red_recv)
    red.src_total = tot
    enter(red.round1 + red.round2)
    red.start(True)
    keeps = [keep_copy(links, new, part, keep_sem) for part in range(4)]

    def hook(i):
        for part in range(3):
            @pl.when(i == (part + 1) * geo.chunks)
            def _():
                per_core(links.c, lambda core: links.forward(OWN, part, core))
                keeps[part].start()

        @pl.when(i == 3 * geo.chunks)
        def _():
            def early(core):
                for slot in (MATE,) if core == 0 else (below(0), above(0)):
                    links.relay(slot, 0, core)
            per_core(links.c, early)

    cube_loop(geo, red, links.r, full_in, sq, strip, new, buf, acc, buf_sem, hook)
    keeps[3].start()
    per_core(links.c, lambda core: complete(geo, links, core, keeps, tin, tout, tsem, 1))


def last_kernel(geo, full_in, sq, strip, sums, ham, dens, energy, new, send_sem, recv_sem, sib_send, sib_recv, keep_sem,
                buf, acc, buf_sem, mid, tot, box, red_send, red_recv, esum, emid, ebox, eother, esend, erecv):
    d, r, c = (lax.axis_index(a) for a in ("depth", "row", "col"))
    blk, strip_rows, layers = geo.blk, geo.strip, geo.layers
    red = Reduce(geo, sums, mid, box, red_send, red_recv)
    red.src_total = tot
    ered = Reduce(geo, esum, emid, ebox, esend, erecv)
    up, down, across = ({"depth": rem(d + k, 4)} for k in (1, 3, 2))
    sibling = {"col": 1 - c}
    enter(red.round1 + [up, down, across, sibling, red.round2[2]])
    red.start(True)
    hh = strip_rows // 2
    slots = {(0, None): 0, (1, None): 1, (3, None): 2, (2, 0): 3, (2, 1): 4}

    def place(delta, who, h, q):
        core = c if who == 0 else 1 - c
        dd = rem(d + delta, 4)
        row0, size = (rem(dd, layers) * 2 + core) * strip_rows, strip_rows
        if h is not None:
            row0, size = row0 + h * hh, hh
        return dens.at[dd // layers, pl.ds(pl.multiple_of(row0, 8), size), pl.ds(q * blk, blk)]

    def cols_of(part):
        return pl.ds(pl.multiple_of(rem(2 * c + part, 4) * blk, LANE), blk)

    def copy(src, dst, there, who, q, dev, n):
        return pltpu.make_async_remote_copy(
            src_ref=src, dst_ref=dst, send_sem=send_sem.at[n, who, q], recv_sem=recv_sem.at[slots[there], who, q],
            device_id=dev, device_id_type=MESH)

    def out_copies(who, q):
        here = place(0, who, None, q)
        src = new.at[:, cols_of(q)] if who == 0 else here
        return [copy(src, here, (3, None), who, q, up, 0), copy(src, here, (1, None), who, q, down, 1)]

    def half_copies(who, q):
        top, low = place(3, who, 0, q), place(1, who, 1, q)
        return [copy(top, top, (2, 0), who, q, up, 2), copy(low, low, (2, 1), who, q, down, 3)]

    def sib_copy(q):
        return pltpu.make_async_remote_copy(
            src_ref=new.at[:, cols_of(2 + q)], dst_ref=place(0, 0, None, q), send_sem=sib_send.at[q],
            recv_sem=sib_recv.at[q], device_id=sibling, device_id_type=MESH)

    def arrive(delta, h, who, q):
        ref = place(delta, who, h, q)
        pltpu.make_async_copy(ref, ref, recv_sem.at[slots[(delta, h)], who, q]).wait()

    keeps = [pltpu.make_async_copy(new.at[:, cols_of(q)], place(0, 0, None, q), keep_sem.at[q]) for q in (0, 1)]

    def relay(who, q):
        halves = half_copies(who, q)
        arrive(3, None, who, q)
        halves[0].start()
        arrive(1, None, who, q)
        halves[1].start()

    def energy_part(part):
        cols = cols_of(part)
        s = jnp.sum(new[:, cols] * ham[:, cols], axis=0, keepdims=True)
        s = jnp.sum(s, axis=1, keepdims=True)
        part_sum = jnp.broadcast_to(s, esum.shape)
        esum[...] = part_sum if part == 0 else esum[...] + part_sum

    def hook(i):
        for part in range(4):
            if part < 3:
                at = i == (part + 1) * geo.chunks

                @pl.when(at)
                def _():
                    if part < 2:
                        for cp in out_copies(0, part):
                            cp.start()
                        keeps[part].start()
                    else:
                        sib_copy(part - 2).start()

            @pl.when(i == (part + 1) * geo.chunks - 1)
            def _():
                energy_part(part)

    cube_loop(geo, red, 2 * c, full_in, sq, strip, new, buf, acc, buf_sem, hook)

    def sibling_out(q):
        ref = place(0, 1, None, q)
        pltpu.make_async_copy(ref, ref, sib_recv.at[q]).wait()
        for cp in out_copies(1, q):
            cp.start()

    sibling_out(0)
    sib_copy(1).start()
    ered.start(True)
    sibling_out(1)
    emid_val = ered.total(True)
    emid[...] = emid_val
    for q in (0, 1):
        relay(0, q)
    ered.start(False)
    for q in (0, 1):
        relay(1, q)
    tot[...] = ered.total(False)
    for who in (0, 1):
        for q in (0, 1):
            for h in (0, 1):
                arrive(2, h, who, q)
    swap = pltpu.make_async_remote_copy(
        src_ref=tot, dst_ref=eother, send_sem=esend.at[6], recv_sem=erecv.at[6], device_id=across, device_id_type=MESH)
    swap.start()
    for cp in keeps:
        cp.wait()
    for who in (0, 1):
        for q in (0, 1):
            for cp in out_copies(who, q) + half_copies(who, q):
                cp.wait_send()
    for q in (0, 1):
        sib_copy(q).wait_send()
    swap.wait()
    mine_first = (d // layers) == 0
    row = lax.broadcasted_iota(jnp.int32, energy.shape, 0)
    a, b = tot[...], eother[...]
    low = jnp.where(mine_first, a, b)
    high = jnp.where(mine_first, b, a)
    energy[...] = 2.0 * jnp.where(row == 0, low, high)


VM = pl.BlockSpec(memory_space=pltpu.VMEM)
ANY = pl.BlockSpec(memory_space=pl.ANY)
DMA = pltpu.SemaphoreType.DMA
TILE = (8, LANE)


def link_scratch(geo):
    return [DMA((9, 3)), DMA((10, 3)), DMA((10, 3)), DMA((10, 3)), DMA((4,)),
            pltpu.VMEM((geo.blk, geo.blk), jnp.float32), pltpu.VMEM((geo.blk, geo.blk), jnp.float32), DMA]


def cube_scratch(geo):
    return [pltpu.VMEM((2, geo.chunk, geo.blk), jnp.float32), pltpu.VMEM((geo.strip, geo.blk), jnp.float32), DMA((2,)),
            pltpu.VMEM(TILE, jnp.float32), pltpu.VMEM(TILE, jnp.float32), pltpu.VMEM((6, *TILE), jnp.float32),
            DMA((6,)), DMA((6,))]


def params(call):
    return pltpu.CompilerParams(collective_id=call, has_side_effects=True)


def first(geo, strip, call):
    return pl.pallas_call(
        functools.partial(first_kernel, geo), name="first",
        out_shape=jax.ShapeDtypeStruct((geo.order, geo.order), jnp.float32),
        in_specs=[VM], out_specs=ANY, scratch_shapes=link_scratch(geo), compiler_params=params(call))(strip)


def middle(geo, full, sq, strip, sums, call):
    return pl.pallas_call(
        functools.partial(mid_kernel, geo), name="middle",
        out_shape=(jax.ShapeDtypeStruct((geo.order, geo.order), jnp.float32),
                   jax.ShapeDtypeStruct((geo.strip, geo.order), jnp.float32)),
        in_specs=[ANY, VM, VM, VM], out_specs=(ANY, VM), scratch_shapes=link_scratch(geo) + cube_scratch(geo),
        compiler_params=params(call))(full, sq, strip, sums)


def last(geo, full, sq, strip, sums, ham, call):
    one = pltpu.VMEM(TILE, jnp.float32)
    return pl.pallas_call(
        functools.partial(last_kernel, geo), name="last",
        out_shape=(jax.ShapeDtypeStruct((geo.kpoints, geo.blk, geo.half), jnp.float32),
                   jax.ShapeDtypeStruct(TILE, jnp.float32)),
        in_specs=[ANY, VM, VM, VM, VM], out_specs=(ANY, VM),
        scratch_shapes=[pltpu.VMEM((geo.strip, geo.order), jnp.float32), DMA((4, 2, 2)), DMA((5, 2, 2)), DMA((2,)), DMA((2,)),
                        DMA((2,))] + cube_scratch(geo) + [one, one, pltpu.VMEM((6, *TILE), jnp.float32), one, DMA((7,)), DMA((7,))],
        compiler_params=params(call))(full, sq, strip, sums, ham)


def solution(mesh):
    def local_purify(ham, spec_bounds, occ_count):
        geo = Geometry(mesh, ham.shape)
        n = geo.order
        d = lax.axis_index("depth")
        r = lax.axis_index("row")
        c = lax.axis_index("col")
        m, e = d // geo.layers, d % geo.layers
        per_col = geo.rows // geo.cols
        on_diag = (r // per_col) == c
        diag_start = (r % per_col) * geo.blk
        square = lax.dynamic_slice_in_dim(ham, diag_start, geo.blk, axis=2)
        tr = jnp.where(on_diag, jnp.trace(square, axis1=1, axis2=2), 0.0)
        mu = lax.psum(tr, ("row", "col")) / n
        occ = occ_count.astype(jnp.float32)
        lam = jnp.minimum(occ / (spec_bounds[:, 1] - mu), (n - occ) / (mu - spec_bounds[:, 0]))
        add = (lam * mu + occ) / n
        scale = lam / n

        row0 = r * geo.blk + (e * 2 + c) * geo.strip
        rows = lax.broadcasted_iota(jnp.int32, (geo.strip, n), 0) + row0
        cols = lax.broadcasted_iota(jnp.int32, (geo.strip, n), 1)
        diag = rows == cols

        ham_m = lax.dynamic_index_in_dim(ham, m, axis=0, keepdims=False)
        layer_rows = lax.dynamic_slice_in_dim(ham_m, e * 2 * geo.strip, 2 * geo.strip, axis=0)
        layer_all = lax.all_gather(layer_rows, "col", axis=1, tiled=True)
        ham_strip = lax.dynamic_slice_in_dim(layer_all, c * geo.strip, geo.strip, axis=0)
        strip = jnp.where(diag, add[m], 0.0) - scale[m] * ham_strip

        full = first(geo, strip, 0)
        for step in range(STEPS):
            sq = jnp.dot(strip, full, precision=HIGHEST, preferred_element_type=jnp.float32)
            sums = jnp.stack([jnp.sum(jnp.where(diag, strip, 0.0)), jnp.sum(strip * strip), jnp.sum(sq * strip)])
            sums = jnp.broadcast_to(jnp.pad(sums, (0, 5))[:, None], TILE)
            if step < STEPS - 1:
                full, strip = middle(geo, full, sq, strip, sums, step + 1)
        density, pair = last(geo, full, sq, strip, sums, ham_strip, STEPS)
        energy = pair[:geo.kpoints, 0]
        return density, energy

    mat = P("spin", "row", "col")
    return jax.shard_map(
        local_purify, mesh=mesh, in_specs=(mat, P("spin", None), P("spin")), out_specs=(mat, P("spin")), check_vma=False)
```

```python
import functools

import jax
import jax.numpy as jnp
from jax import lax
from jax.experimental import pallas as pl
from jax.experimental.pallas import tpu as pltpu
from jax.sharding import PartitionSpec as P

STEPS = 3
MESH = pl.DeviceIdType.MESH
LANE = 128
HIGHEST = lax.Precision.HIGHEST


class Geometry:
    def __init__(self, mesh, ham_shape):
        kpoints, self.blk, self.half = ham_shape
        self.depth = mesh.shape["depth"]
        self.rows = mesh.shape["row"]
        self.cols = mesh.shape["col"]
        self.kpoints = kpoints
        self.layers = self.depth // kpoints
        self.order = self.half * self.cols
        self.strip = self.blk // (self.layers * self.cols)
        self.lo = self.blk // 2 // LANE * LANE
        self.wide = self.blk - self.lo
        self.chunk = 4 * LANE
        self.chunks = self.order // self.chunk
        assert self.rows == 4 and self.cols == 2 and self.layers == 2 and self.depth == 4


def rem(a, b):
    return lax.rem(a, b)


class Links:
    def __init__(self, geo, own_ref, full_ref, send_sem, recv_sem, sib_send, sib_recv):
        self.geo, self.own, self.full = geo, own_ref, full_ref
        self.send_sem, self.recv_sem, self.sib_send, self.sib_recv = send_sem, recv_sem, sib_send, sib_recv
        d = lax.axis_index("depth")
        self.r = lax.axis_index("row")
        self.c = lax.axis_index("col")
        self.e = rem(d, geo.layers)
        self.up, self.down = {"row": rem(self.r + 1, 4)}, {"row": rem(self.r + 3, 4)}
        self.mate = {"depth": d + 1 - 2 * self.e}
        self.sibling = {"col": 1 - self.c}
        self.drained = set()
        self.slots = {slot: i for i, slot in enumerate(
            [(lam, delta, h) for lam in (0, 1) for delta, h in ((0, None), (1, None), (3, None), (2, 0), (2, 1))])}

    def place(self, slot, part, core):
        geo = self.geo
        lam, delta, h = slot
        rr = rem(self.r + delta, 4)
        ee = self.e if lam == 0 else 1 - self.e
        row0 = rr * geo.blk + (ee * 2 + core) * geo.strip
        size = geo.strip
        if h is not None:
            row0, size = row0 + h * (geo.strip // 2), geo.strip // 2
        if part < 2:
            col0, width = rem(rr + part, 4) * geo.blk, geo.blk
        else:
            col0 = rem(rr + 2, 4) * geo.blk + geo.lo * rem(rr // 2 + ee, 2)
            width = geo.wide
        return pl.ds(pl.multiple_of(row0, 8), size), pl.ds(pl.multiple_of(col0, LANE), width)

    def copy(self, src, there, dev, part, core, n):
        here = self.place(src, part, core)
        ref = self.own.at[:, here[1]] if src == OWN else self.full.at[here]
        return pltpu.make_async_remote_copy(
            src_ref=ref, dst_ref=self.full.at[here], send_sem=self.send_sem.at[n, part],
            recv_sem=self.recv_sem.at[self.slots[there], part], device_id=dev, device_id_type=MESH)

    def sib_copy(self, slot, part, core):
        here = self.place(slot, part, core)
        ref = self.own.at[:, here[1]] if slot == OWN else self.full.at[here]
        i = self.slots[slot]
        return pltpu.make_async_remote_copy(
            src_ref=ref, dst_ref=self.full.at[here], send_sem=self.sib_send.at[i, part],
            recv_sem=self.sib_recv.at[i, part], device_id=self.sibling, device_id_type=MESH)

    def arrive(self, slot, part, core):
        here = self.full.at[self.place(slot, part, core)]
        pltpu.make_async_copy(here, here, self.recv_sem.at[self.slots[slot], part]).wait()

    def sib_arrive(self, slot, part, core):
        here = self.full.at[self.place(slot, part, 1 - core)]
        pltpu.make_async_copy(here, here, self.sib_recv.at[self.slots[slot], part]).wait()

    def sends(self, core):
        table = [(OWN, MATE, self.mate), (OWN, below(0), self.up), (OWN, above(0), self.down)]
        lams = (0, 1) if core == 0 else (0,)
        if core == 0:
            table += [(MATE, below(1), self.up), (MATE, above(1), self.down)]
        for lam in lams:
            table += [((lam, 3, 0), far(lam, 0), self.up), ((lam, 1, 1), far(lam, 1), self.down)]
        if core == 1:
            table += [(below(0), below(1), self.mate), (above(0), above(1), self.mate)]
            table += [(far(0, h), far(1, h), self.mate) for h in (0, 1)]
        return table

    def forward(self, slot, part, core):
        for n, (src, there, dev) in enumerate(self.sends(core)):
            if src == slot or (slot[2] is None and slot[1] in (1, 3) and src[:2] == slot[:2] and src[2] is not None):
                self.copy(src, there, dev, part, core, n).start()
        self.sib_copy(slot, part, core).start()

    def relay(self, slot, part, core):
        self.arrive(slot, part, core)
        self.forward(slot, part, core)

    def drain(self, slots, parts, core):
        for part in parts:
            for n, (src, there, dev) in enumerate(self.sends(core)):
                whole = src[:2] + ((None,) if src[1] != 2 else (src[2],))
                if whole in slots and (core, n, part) not in self.drained:
                    self.drained.add((core, n, part))
                    self.copy(src, there, dev, part, core, n).wait_send()
            for slot in slots:
                if (core, slot, part) not in self.drained:
                    self.drained.add((core, slot, part))
                    self.sib_copy(slot, part, core).wait_send()


OWN, MATE = (0, 0, None), (1, 0, None)


def below(lam):
    return (lam, 3, None)


def above(lam):
    return (lam, 1, None)


def far(lam, h):
    return (lam, 2, h)


def per_core(c, fn):
    pl.when(c == 0)(lambda: fn(0))
    pl.when(c == 1)(lambda: fn(1))


class Reduce:
    def __init__(self, geo, src, mid, box, send, recv):
        self.src, self.mid, self.box, self.send, self.recv = src, mid, box, send, recv
        d, r, c = (lax.axis_index(a) for a in ("depth", "row", "col"))
        mate = d + 1 - 2 * rem(d, geo.layers)
        self.round1 = [{"row": rem(r + k, 4)} for k in (1, 2, 3)]
        self.round2 = [{"depth": mate}, {"col": 1 - c}, {"depth": mate, "col": 1 - c}]

    def copies(self, first):
        devs, src, base = (self.round1, self.src, 0) if first else (self.round2, self.mid, 3)
        return [pltpu.make_async_remote_copy(
            src_ref=src, dst_ref=self.box.at[base + i], send_sem=self.send.at[base + i], recv_sem=self.recv.at[base + i],
            device_id=dev, device_id_type=MESH) for i, dev in enumerate(devs)]

    def start(self, first):
        for cp in self.copies(first):
            cp.start()

    def total(self, first):
        for cp in self.copies(first):
            cp.wait()
        base = 0 if first else 3
        src = self.src if first else self.mid
        return (src[...] + self.box[base]) + (self.box[base + 1] + self.box[base + 2])


def enter(devs):
    barrier = pltpu.get_barrier_semaphore()
    for dev in devs:
        pl.semaphore_signal(barrier, inc=1, device_id=dev, device_id_type=MESH)
    pl.semaphore_wait(barrier, len(devs))


class Mirror:
    def __init__(self, geo, full, tin, tout, fin, fout, sem):
        self.geo, self.full, self.tin, self.tout, self.fin, self.fout, self.sem = geo, full, tin, tout, fin, fout, sem

    def next(self, k):
        geo, blk = self.geo, self.geo.blk
        row0, col0 = rem(k, 4) * blk, rem(k + 1, 4) * blk
        slabs = blk // LANE

        def load(t):
            rows = pl.ds(pl.multiple_of(row0 + t * LANE, LANE), LANE)
            return pltpu.make_async_copy(
                self.full.at[rows, pl.ds(pl.multiple_of(col0, LANE), blk)],
                self.tin.at[pl.ds(pl.multiple_of(t * LANE, LANE), LANE)], self.sem.at[0, t])

        def store(t):
            cols = pl.ds(pl.multiple_of(row0 + t * LANE, LANE), LANE)
            return pltpu.make_async_copy(
                self.tout.at[:, pl.ds(pl.multiple_of(t * LANE, LANE), LANE)],
                self.full.at[pl.ds(pl.multiple_of(col0, LANE), blk), cols], self.sem.at[1, t])

        def turn(t):
            load(t).wait()
            at = pl.ds(pl.multiple_of(t * LANE, LANE), LANE)
            self.tout[:, at] = self.tin[at, :].T
            store(t).start()

        self.each(slabs, lambda t: load(t).start())
        self.each(slabs, turn)
        self.each(slabs, lambda t: store(t).wait())

    def far(self, k):
        geo = self.geo

        def place(j):
            i, t = rem(k + 2 * (j // 2), 4), rem(j, 2)
            row0 = i * geo.blk + t * geo.wide
            col0 = rem(i + 2, 4) * geo.blk + geo.lo * rem(i // 2 + t, 2)
            return pl.multiple_of(row0, LANE), pl.multiple_of(col0, LANE)

        def load(j):
            row0, col0 = place(j)
            return pltpu.make_async_copy(
                self.full.at[pl.ds(row0, geo.lo), pl.ds(col0, geo.wide)], self.fin.at[j], self.sem.at[0, j])

        def store(j):
            row0, col0 = place(j)
            return pltpu.make_async_copy(
                self.fout.at[j], self.full.at[pl.ds(col0, geo.wide), pl.ds(row0, geo.lo)], self.sem.at[1, j])

        def turn(j):
            load(j).wait()
            for t in range(geo.lo // LANE):
                at = slice(t * LANE, (t + 1) * LANE)
                self.fout[j, :, at] = self.fin[j, at, :].T
            store(j).start()

        self.each(4, lambda j: load(j).start())
        self.each(4, turn)
        self.each(4, lambda j: store(j).wait())

    @staticmethod
    def each(count, fn):
        def body(t, carry):
            fn(t)
            return carry

        lax.fori_loop(0, count, body, 0)


def complete(links, core, keeps, mirror, done):
    r = links.r
    near = (MATE,) if core == 0 else (below(0), above(0))
    for part in range(done, 3):
        for slot in near:
            links.relay(slot, part, core)
    if core == 0:
        for lam in (0, 1):
            for part in range(3):
                links.relay(below(lam), part, core)
                links.relay(above(lam), part, core)
    else:
        for part in range(3):
            links.relay(MATE, part, core)
        for part in range(3):
            for h in (0, 1):
                links.relay(far(0, h), part, core)
    for cp in keeps:
        cp.wait()

    def sibs(slots, parts=range(3)):
        for slot in slots:
            for part in parts:
                links.sib_arrive(slot, part, core)

    def far_relays(lam, parts):
        for part in parts:
            for h in (0, 1):
                links.relay(far(lam, h), part, core)

    near = (below(0), below(1), above(0), above(1))
    fars = [far(lam, h) for lam in (0, 1) for h in (0, 1)]
    sibs((OWN, MATE))
    mirror.next(r)
    if core == 1:
        for part in range(3):
            links.relay(below(1), part, core)
            links.relay(above(1), part, core)
    sibs(near)
    mirror.next(r + 3)
    if core == 0:
        far_relays(0, range(3))
    far_relays(1, (0,))
    mirror.next(r + 1)
    far_relays(1, (1,))
    links.drain(near, (2,), core)
    mirror.far(r + 1)
    far_relays(1, (2,))
    sibs(fars, (0, 1))
    mirror.next(r + 2)
    sibs(fars, (2,))
    links.drain((OWN, MATE, *fars), (2,), core)
    mirror.far(r)
    links.drain(list(links.slots), range(3), core)


def keep_copy(links, own, part, sem):
    geo = links.geo
    row0 = links.r * geo.blk + (links.e * 2 + links.c) * geo.strip
    cols = pl.ds(pl.multiple_of(rem(links.r + part, 4) * geo.blk, LANE), geo.blk)
    return pltpu.make_async_copy(own.at[:, cols], links.full.at[pl.ds(pl.multiple_of(row0, 8), geo.strip), cols], sem.at[part])


def first_kernel(geo, ham, part_trace, bounds, strip, full, send_sem, recv_sem, sib_send, sib_recv, keep_sem, tin, tout, fin,
                 fout, tsem, mid, tot, box, red_send, red_recv):
    links = Links(geo, strip, full, send_sem, recv_sem, sib_send, sib_recv)
    red = Reduce(geo, part_trace, mid, box, red_send, red_recv)
    enter(red.round1 + red.round2)
    red.start(True)
    mid[...] = red.total(True)
    strip[...] = -ham[...]
    red.start(False)
    tot[...] = red.total(False)
    n = geo.order
    mu = tot[0:1, 0:1] / n
    occ, low, high = (bounds[j:j + 1, 0:1] for j in range(3))
    lam = jnp.minimum(occ / (high - mu), (n - occ) / (mu - low))
    add, scale = (lam * mu + occ) / n, lam / n
    row0 = links.r * geo.blk + (links.e * 2 + links.c) * geo.strip

    def shift(t, carry):
        cols = pl.ds(pl.multiple_of(t * LANE, LANE), LANE)
        shape = (geo.strip, LANE)
        diag = (lax.broadcasted_iota(jnp.int32, shape, 0) + row0) == (lax.broadcasted_iota(jnp.int32, shape, 1) + t * LANE)
        strip[:, cols] = jnp.where(diag, add, 0.0) + scale * strip[:, cols]
        return carry

    lax.fori_loop(0, n // LANE, shift, 0)
    keeps = [keep_copy(links, strip, part, keep_sem) for part in range(4)]

    def run(core):
        for cp in keeps:
            cp.start()
        for part in range(3):
            links.forward(OWN, part, core)
        complete(links, core, keeps, Mirror(geo, full, tin, tout, fin, fout, tsem), 0)

    per_core(links.c, run)


def cube_loop(geo, red, first_block, full_in, sq, strip, new, buf, acc, buf_sem, hook):
    per, size, blk = geo.chunks, geo.chunk, geo.blk

    def cols_of(part):
        return pl.ds(pl.multiple_of(rem(first_block + part, 4) * blk, LANE), blk)

    def load(i):
        rows = pl.ds(pl.multiple_of(rem(i, per) * size, LANE), size)
        slot = rem(i, 2)
        return pltpu.make_async_copy(full_in.at[rows, cols_of(i // per)], buf.at[slot], buf_sem.at[slot])

    load(0).start()

    def body(i, carry):
        k = rem(i, per)

        @pl.when(i + 1 < 4 * per)
        def _():
            load(i + 1).start()

        load(i).wait()

        @pl.when(k == 0)
        def _():
            acc[...] = jnp.zeros_like(acc)

        acc[...] += jnp.dot(sq[:, pl.ds(pl.multiple_of(k * size, LANE), size)], buf[rem(i, 2)],
                            precision=HIGHEST, preferred_element_type=jnp.float32)

        @pl.when(i == 1)
        def _():
            red.mid[...] = red.total(True)

        @pl.when(i == 3)
        def _():
            red.start(False)

        @pl.when(i == per - 1)
        def _():
            red.src_total[...] = red.total(False)

        @pl.when(k == per - 1)
        def _():
            cols = cols_of(i // per)
            t1, t2, t3 = (red.src_total[j:j + 1, 0:1] for j in range(3))
            coef = (t2 - t3) / (t1 - t2)
            new[:, cols] = ((1.0 - 2.0 * coef) * strip[:, cols] + (1.0 + coef) * sq[:, cols] - acc[...]) / (1.0 - coef)

        hook(i)
        return carry

    lax.fori_loop(0, 4 * per, body, 0)


def mid_kernel(geo, full_in, sq, strip, sums, full, new, send_sem, recv_sem, sib_send, sib_recv, keep_sem, tin, tout, fin, fout,
               tsem, buf, acc, buf_sem, mid, tot, box, red_send, red_recv):
    links = Links(geo, new, full, send_sem, recv_sem, sib_send, sib_recv)
    mirror = Mirror(geo, full, tin, tout, fin, fout, tsem)
    red = Reduce(geo, sums, mid, box, red_send, red_recv)
    red.src_total = tot
    enter(red.round1 + red.round2)
    red.start(True)
    keeps = [keep_copy(links, new, part, keep_sem) for part in range(4)]

    def hook(i):
        for part in range(3):
            @pl.when(i == (part + 1) * geo.chunks)
            def _():
                per_core(links.c, lambda core: links.forward(OWN, part, core))
                keeps[part].start()

        @pl.when(i == 3 * geo.chunks)
        def _():
            def early(core):
                for slot in (MATE,) if core == 0 else (below(0), above(0)):
                    links.relay(slot, 0, core)
            per_core(links.c, early)

    cube_loop(geo, red, links.r, full_in, sq, strip, new, buf, acc, buf_sem, hook)
    keeps[3].start()
    per_core(links.c, lambda core: complete(links, core, keeps, mirror, 1))


def last_kernel(geo, full_in, sq, strip, sums, ham, dens, energy, new, send_sem, recv_sem, sib_send, sib_recv, keep_sem,
                buf, acc, buf_sem, mid, tot, box, red_send, red_recv, esum, emid, ebox, eother, esend, erecv):
    d, r, c = (lax.axis_index(a) for a in ("depth", "row", "col"))
    blk, strip_rows, layers = geo.blk, geo.strip, geo.layers
    red = Reduce(geo, sums, mid, box, red_send, red_recv)
    red.src_total = tot
    ered = Reduce(geo, esum, emid, ebox, esend, erecv)
    up, down, across = ({"depth": rem(d + k, 4)} for k in (1, 3, 2))
    sibling = {"col": 1 - c}
    enter(red.round1 + [up, down, across, sibling, red.round2[2]])
    red.start(True)
    hh = strip_rows // 2
    slots = {(0, None): 0, (1, None): 1, (3, None): 2, (2, 0): 3, (2, 1): 4}

    def place(delta, who, h, q):
        core = c if who == 0 else 1 - c
        dd = rem(d + delta, 4)
        row0, size = (rem(dd, layers) * 2 + core) * strip_rows, strip_rows
        if h is not None:
            row0, size = row0 + h * hh, hh
        return dens.at[dd // layers, pl.ds(pl.multiple_of(row0, 8), size), pl.ds(q * blk, blk)]

    def cols_of(part):
        return pl.ds(pl.multiple_of(rem(2 * c + part, 4) * blk, LANE), blk)

    def copy(src, dst, there, who, q, dev, n):
        return pltpu.make_async_remote_copy(
            src_ref=src, dst_ref=dst, send_sem=send_sem.at[n, who, q], recv_sem=recv_sem.at[slots[there], who, q],
            device_id=dev, device_id_type=MESH)

    def out_copies(who, q):
        here = place(0, who, None, q)
        src = new.at[:, cols_of(q)] if who == 0 else here
        return [copy(src, here, (3, None), who, q, up, 0), copy(src, here, (1, None), who, q, down, 1)]

    def half_copies(who, q):
        top, low = place(3, who, 0, q), place(1, who, 1, q)
        return [copy(top, top, (2, 0), who, q, up, 2), copy(low, low, (2, 1), who, q, down, 3)]

    def sib_copy(q):
        return pltpu.make_async_remote_copy(
            src_ref=new.at[:, cols_of(2 + q)], dst_ref=place(0, 0, None, q), send_sem=sib_send.at[q],
            recv_sem=sib_recv.at[q], device_id=sibling, device_id_type=MESH)

    def arrive(delta, h, who, q):
        ref = place(delta, who, h, q)
        pltpu.make_async_copy(ref, ref, recv_sem.at[slots[(delta, h)], who, q]).wait()

    keeps = [pltpu.make_async_copy(new.at[:, cols_of(q)], place(0, 0, None, q), keep_sem.at[q]) for q in (0, 1)]

    def relay(who, q):
        halves = half_copies(who, q)
        arrive(3, None, who, q)
        halves[0].start()
        arrive(1, None, who, q)
        halves[1].start()

    def energy_part(part):
        cols = cols_of(part)
        s = jnp.sum(new[:, cols] * ham[:, cols], axis=0, keepdims=True)
        s = jnp.sum(s, axis=1, keepdims=True)
        part_sum = jnp.broadcast_to(s, esum.shape)
        esum[...] = part_sum if part == 0 else esum[...] + part_sum

    def hook(i):
        for part in range(4):
            if part < 3:
                at = i == (part + 1) * geo.chunks

                @pl.when(at)
                def _():
                    if part < 2:
                        for cp in out_copies(0, part):
                            cp.start()
                        keeps[part].start()
                    else:
                        sib_copy(part - 2).start()

            @pl.when(i == (part + 1) * geo.chunks - 1)
            def _():
                energy_part(part)

    cube_loop(geo, red, 2 * c, full_in, sq, strip, new, buf, acc, buf_sem, hook)

    def sibling_out(q):
        ref = place(0, 1, None, q)
        pltpu.make_async_copy(ref, ref, sib_recv.at[q]).wait()
        for cp in out_copies(1, q):
            cp.start()

    sibling_out(0)
    sib_copy(1).start()
    ered.start(True)
    sibling_out(1)
    emid_val = ered.total(True)
    emid[...] = emid_val
    for q in (0, 1):
        relay(0, q)
    ered.start(False)
    for q in (0, 1):
        relay(1, q)
    tot[...] = ered.total(False)
    for who in (0, 1):
        for q in (0, 1):
            for h in (0, 1):
                arrive(2, h, who, q)
    swap = pltpu.make_async_remote_copy(
        src_ref=tot, dst_ref=eother, send_sem=esend.at[6], recv_sem=erecv.at[6], device_id=across, device_id_type=MESH)
    swap.start()
    for cp in keeps:
        cp.wait()
    for who in (0, 1):
        for q in (0, 1):
            for cp in out_copies(who, q) + half_copies(who, q):
                cp.wait_send()
    for q in (0, 1):
        sib_copy(q).wait_send()
    swap.wait()
    mine_first = (d // layers) == 0
    row = lax.broadcasted_iota(jnp.int32, energy.shape, 0)
    a, b = tot[...], eother[...]
    low = jnp.where(mine_first, a, b)
    high = jnp.where(mine_first, b, a)
    energy[...] = 2.0 * jnp.where(row == 0, low, high)


VM = pl.BlockSpec(memory_space=pltpu.VMEM)
ANY = pl.BlockSpec(memory_space=pl.ANY)
DMA = pltpu.SemaphoreType.DMA
TILE = (8, LANE)


def link_scratch(geo):
    return [DMA((9, 3)), DMA((10, 3)), DMA((10, 3)), DMA((10, 3)), DMA((4,)),
            pltpu.VMEM((geo.blk, geo.blk), jnp.float32), pltpu.VMEM((geo.blk, geo.blk), jnp.float32),
            pltpu.VMEM((4, geo.lo, geo.wide), jnp.float32), pltpu.VMEM((4, geo.wide, geo.lo), jnp.float32), DMA((2, max(4, geo.blk // LANE)))]


def cube_scratch(geo):
    return [pltpu.VMEM((2, geo.chunk, geo.blk), jnp.float32), pltpu.VMEM((geo.strip, geo.blk), jnp.float32), DMA((2,)),
            pltpu.VMEM(TILE, jnp.float32), pltpu.VMEM(TILE, jnp.float32), pltpu.VMEM((6, *TILE), jnp.float32),
            DMA((6,)), DMA((6,))]


def params(call):
    return pltpu.CompilerParams(collective_id=call, has_side_effects=True)


def first(geo, ham, part_trace, bounds, call):
    return pl.pallas_call(
        functools.partial(first_kernel, geo), name="first",
        out_shape=(jax.ShapeDtypeStruct((geo.strip, geo.order), jnp.float32),
                   jax.ShapeDtypeStruct((geo.order, geo.order), jnp.float32)),
        in_specs=[VM, VM, VM], out_specs=(VM, ANY), scratch_shapes=link_scratch(geo) + cube_scratch(geo)[3:],
        compiler_params=params(call))(ham, part_trace, bounds)


def middle(geo, full, sq, strip, sums, call):
    return pl.pallas_call(
        functools.partial(mid_kernel, geo), name="middle",
        out_shape=(jax.ShapeDtypeStruct((geo.order, geo.order), jnp.float32),
                   jax.ShapeDtypeStruct((geo.strip, geo.order), jnp.float32)),
        in_specs=[ANY, VM, VM, VM], out_specs=(ANY, VM), scratch_shapes=link_scratch(geo) + cube_scratch(geo),
        compiler_params=params(call))(full, sq, strip, sums)


def last(geo, full, sq, strip, sums, ham, call):
    one = pltpu.VMEM(TILE, jnp.float32)
    return pl.pallas_call(
        functools.partial(last_kernel, geo), name="last",
        out_shape=(jax.ShapeDtypeStruct((geo.kpoints, geo.blk, geo.half), jnp.float32),
                   jax.ShapeDtypeStruct(TILE, jnp.float32)),
        in_specs=[ANY, VM, VM, VM, VM], out_specs=(ANY, VM),
        scratch_shapes=[pltpu.VMEM((geo.strip, geo.order), jnp.float32), DMA((4, 2, 2)), DMA((5, 2, 2)), DMA((2,)), DMA((2,)),
                        DMA((2,))] + cube_scratch(geo) + [one, one, pltpu.VMEM((6, *TILE), jnp.float32), one, DMA((7,)), DMA((7,))],
        compiler_params=params(call))(full, sq, strip, sums, ham)


def solution(mesh):
    def local_purify(ham, spec_bounds, occ_count):
        geo = Geometry(mesh, ham.shape)
        n = geo.order
        d = lax.axis_index("depth")
        r = lax.axis_index("row")
        c = lax.axis_index("col")
        m, e = d // geo.layers, d % geo.layers
        row0 = r * geo.blk + (e * 2 + c) * geo.strip
        rows = lax.broadcasted_iota(jnp.int32, (geo.strip, n), 0) + row0
        cols = lax.broadcasted_iota(jnp.int32, (geo.strip, n), 1)
        diag = rows == cols

        ham_m = lax.dynamic_index_in_dim(ham, m, axis=0, keepdims=False)
        own = lax.dynamic_slice_in_dim(ham_m, (e * 2 + c) * geo.strip, geo.strip, axis=0)
        theirs = lax.dynamic_slice_in_dim(ham_m, (e * 2 + 1 - c) * geo.strip, geo.strip, axis=0)
        got = lax.ppermute(theirs, "col", [(0, 1), (1, 0)])
        ham_strip = jnp.concatenate([jnp.where(c == 0, own, got), jnp.where(c == 0, got, own)], axis=1)
        tile = lambda rows: jnp.broadcast_to(jnp.pad(jnp.stack(rows), (0, 8 - len(rows)))[:, None], TILE)
        trace = tile([jnp.sum(jnp.where(diag, ham_strip, 0.0))])
        bounds = tile([occ_count[m].astype(jnp.float32), spec_bounds[m, 0], spec_bounds[m, 1]])
        strip, full = first(geo, ham_strip, trace, bounds, 0)
        for step in range(STEPS):
            sq = jnp.dot(strip, full, precision=HIGHEST, preferred_element_type=jnp.float32)
            sums = tile([jnp.sum(jnp.where(diag, strip, 0.0)), jnp.sum(strip * strip), jnp.sum(sq * strip)])
            if step < STEPS - 1:
                full, strip = middle(geo, full, sq, strip, sums, step + 1)
        density, pair = last(geo, full, sq, strip, sums, ham_strip, STEPS)
        energy = pair[:geo.kpoints, 0]
        return density, energy

    mat = P("spin", "row", "col")
    return jax.shard_map(
        local_purify, mesh=mesh, in_specs=(mat, P("spin", None), P("spin")), out_specs=(mat, P("spin")), check_vma=False)
```
